16 devices in a mesh: dp: 2 (over z), sp: 8 (over y, x, core).
Axes of the slice: x: 2, y: 2, z: 2, core: 2. Of those that a mesh axis runs over, the one named last changes fastest.
Arguments:
- x: bfloat16 [2, 4096, 3584], P('dp', 'sp'), parts along dimension 0
- segment_ids: int32 [2, 4096], P('dp', 'sp'), parts along dimension 0
- positions: int32 [2, 4096], P('dp', 'sp'), parts along dimension 0
- out_grad: bfloat16 [2, 4096, 3584], P('dp', 'sp'), parts along dimension 0
- norm_scale: bfloat16 [3584], replicated
- w_q: bfloat16 [3584, 4096], replicated
- w_k: bfloat16 [3584, 256], replicated
- w_v: bfloat16 [3584, 256], replicated
- w_o: bfloat16 [4096, 3584], replicated
- b_o: bfloat16 [3584], replicated
Outputs:
- output 1: bfloat16 [2, 4096, 3584], P('dp', 'sp'), parts along dimension 0
- output 2: bfloat16 [2, 4096, 3584], P('dp', 'sp'), parts along dimension 0
- output 3: bfloat16 [7168], P('dp'), parts along dimension 0
- output 4: bfloat16 [7168, 4096], P('dp'), parts along dimension 0
- output 5: bfloat16 [7168, 256], P('dp'), parts along dimension 0
- output 6: bfloat16 [7168, 256], P('dp'), parts along dimension 0
- output 7: bfloat16 [8192, 3584], P('dp'), parts along dimension 0
- output 8: bfloat16 [7168], P('dp'), parts along dimension 0
There are 2 independent parts. The reference program is written for one: setup_inputs(seed, part) draws one part's arguments, and reference() takes and returns one part's arrays. A program takes and returns all parts, laid end to end along the dimension named above; an argument that names none is the same for every part.
All inputs are finite; a program needn't handle non-finite values.
Results may differ from the reference program's by a relative error of at most 0.0176995.
Values are sent between devices in bfloat16 or wider.
A program may use at most 1 GiB of HBM per device.

```python
import jax
import jax.numpy as jnp
from jax import lax

BATCH_SIZE = 1
SEQ_LEN = 4096
MODEL_DIM = 3584
NUM_HEADS = 16
HEAD_DIM = 256
WINDOW = 2048
QUERY_BLOCK = 128
DOC_MEAN = max(QUERY_BLOCK, min(2 * WINDOW, SEQ_LEN // 4))
QK_GAIN = 1.7
NORM_EPS = 1e-6
ROPE_BASE = 10000.0
NEG_BIG = -1e30


def draw_documents(start_key, offset_key):
    token_idx = jnp.arange(SEQ_LEN, dtype=jnp.int32)[None, :]
    starts = jax.random.randint(start_key, (BATCH_SIZE, SEQ_LEN), 0, DOC_MEAN) == 0
    starts = starts & (token_idx > 0)
    seg_ids = jnp.cumsum(starts.astype(jnp.int32), axis=1).astype(jnp.int32)
    doc_start = lax.cummax(jnp.where(starts, token_idx, 0), axis=1)
    row_offset = jax.random.randint(offset_key, (BATCH_SIZE, 1), 0, 4096)
    positions = (token_idx - doc_start + row_offset).astype(jnp.int32)
    return seg_ids, positions


def setup_inputs(seed: int = 0, part: int = 0) -> dict:
    shared_keys = jax.random.split(jax.random.key(seed), 7)
    part_keys = jax.random.split(jax.random.fold_in(jax.random.key(seed + 1), part), 4)
    seg_ids, positions = draw_documents(part_keys[2], part_keys[3])
    act_shape = (BATCH_SIZE, SEQ_LEN, MODEL_DIM)
    q_width = NUM_HEADS * HEAD_DIM
    in_std = MODEL_DIM ** -0.5

    def normal_bf16(rng_key, shape, std_dev):
        return (jax.random.normal(rng_key, shape, jnp.float32) * std_dev).astype(jnp.bfloat16)

    return {
        "x": normal_bf16(part_keys[0], act_shape, 1.0),
        "segment_ids": seg_ids,
        "positions": positions,
        "out_grad": normal_bf16(part_keys[1], act_shape, 1.0),
        "norm_scale": normal_bf16(shared_keys[0], (MODEL_DIM,), 0.3),
        "w_q": normal_bf16(shared_keys[1], (MODEL_DIM, q_width), QK_GAIN * in_std),
        "w_k": normal_bf16(shared_keys[2], (MODEL_DIM, HEAD_DIM), QK_GAIN * in_std),
        "w_v": normal_bf16(shared_keys[3], (MODEL_DIM, HEAD_DIM), in_std),
        "w_o": normal_bf16(shared_keys[4], (q_width, MODEL_DIM), q_width ** -0.5),
        "b_o": normal_bf16(shared_keys[5], (MODEL_DIM,), 0.3),
    }


def rms_norm(x_f32, norm_gain):
    mean_sq = jnp.mean(x_f32 * x_f32, axis=-1, keepdims=True)
    return (x_f32 * lax.rsqrt(mean_sq + NORM_EPS) * (1.0 + norm_gain.astype(jnp.float32))).astype(jnp.bfloat16)


def rotary(head_vals, positions):
    rot_dim = HEAD_DIM // 2
    half_dim = rot_dim // 2
    inv_freq = ROPE_BASE ** (-(jnp.arange(half_dim, dtype=jnp.float32) * 2.0 / rot_dim))
    angles = positions.astype(jnp.float32)[:, :, None, None] * inv_freq
    cos_a = jnp.cos(angles)
    sin_a = jnp.sin(angles)
    first_half = head_vals[..., :half_dim]
    second_half = head_vals[..., half_dim:rot_dim]
    return jnp.concatenate([first_half * cos_a - second_half * sin_a, second_half * cos_a + first_half * sin_a, head_vals[..., rot_dim:]], axis=-1)


def attention(queries, keys_in, values_in, seg_ids):
    batch_rows, seq_len, n_heads, head_dim = queries.shape
    key_span = WINDOW + QUERY_BLOCK
    keys_pad = jnp.pad(keys_in, ((0, 0), (WINDOW, 0), (0, 0)))
    values_pad = jnp.pad(values_in, ((0, 0), (WINDOW, 0), (0, 0)))
    seg_pad = jnp.pad(seg_ids, ((0, 0), (WINDOW, 0)), constant_values=-1)
    offsets = jnp.arange(key_span)[None, :]
    row_idx = jnp.arange(QUERY_BLOCK)[:, None]
    in_band = (offsets > row_idx) & (offsets <= row_idx + WINDOW)

    def one_block(q_start):
        q_blk = lax.dynamic_slice_in_dim(queries, q_start, QUERY_BLOCK, axis=1)
        k_blk = lax.dynamic_slice_in_dim(keys_pad, q_start, key_span, axis=1)
        v_blk = lax.dynamic_slice_in_dim(values_pad, q_start, key_span, axis=1)
        q_seg = lax.dynamic_slice_in_dim(seg_ids, q_start, QUERY_BLOCK, axis=1)
        k_seg = lax.dynamic_slice_in_dim(seg_pad, q_start, key_span, axis=1)
        allowed = (q_seg[:, :, None] == k_seg[:, None, :]) & in_band[None]
        scores = jnp.einsum("bqhe,bke->bhqk", q_blk.astype(jnp.float32), k_blk.astype(jnp.float32))
        scores = jnp.where(allowed[:, None], scores, NEG_BIG)
        attn_prob = jax.nn.softmax(scores, axis=-1).astype(jnp.bfloat16)
        o_blk = jnp.einsum("bhqk,bke->bqhe", attn_prob.astype(jnp.float32), v_blk.astype(jnp.float32))
        return o_blk.astype(jnp.bfloat16)

    blocks = lax.map(jax.checkpoint(one_block), jnp.arange(seq_len // QUERY_BLOCK) * QUERY_BLOCK)
    return jnp.moveaxis(blocks, 0, 1).reshape(batch_rows, seq_len, n_heads, head_dim)


def forward(x, norm_scale, w_q, w_k, w_v, w_o, b_o, seg_ids, positions):
    x_f32 = x.astype(jnp.float32)
    normed = rms_norm(x_f32, norm_scale)
    q_lin = jnp.dot(normed, w_q, preferred_element_type=jnp.float32).reshape(BATCH_SIZE, SEQ_LEN, NUM_HEADS, HEAD_DIM)
    queries = (rotary(q_lin, positions) * HEAD_DIM ** -0.5).astype(jnp.bfloat16)
    keys_all = rotary(jnp.dot(normed, w_k, preferred_element_type=jnp.float32)[:, :, None, :], positions)[:, :, 0, :].astype(jnp.bfloat16)
    values_all = jnp.dot(normed, w_v, preferred_element_type=jnp.float32).astype(jnp.bfloat16)
    attn_out = attention(queries, keys_all, values_all, seg_ids)
    y_proj = jnp.dot(attn_out.reshape(BATCH_SIZE, SEQ_LEN, NUM_HEADS * HEAD_DIM), w_o, preferred_element_type=jnp.float32)
    return (x_f32 + y_proj + b_o.astype(jnp.float32)).astype(jnp.bfloat16)


def reference(x, segment_ids, positions, out_grad, norm_scale, w_q, w_k, w_v, w_o, b_o):
    def block_fn(x_in, gain_in, wq_in, wk_in, wv_in, wo_in, bo_in):
        return forward(x_in, gain_in, wq_in, wk_in, wv_in, wo_in, bo_in, segment_ids, positions)

    block_out, pull_back = jax.vjp(block_fn, x, norm_scale, w_q, w_k, w_v, w_o, b_o)
    all_grads = pull_back(out_grad)
    return (block_out, all_grads[0], all_grads[1], all_grads[2], all_grads[3], all_grads[4], all_grads[5], all_grads[6])
```

```python
import jax
import jax.numpy as jnp
from jax import lax
from jax.experimental import pallas as pl
from jax.experimental.pallas import tpu as pltpu
from jax.sharding import PartitionSpec as P


WINDOW = 2048
NORM_EPS = 1e-6
ROPE_BASE = 10000.0
NEG_BIG = -1e30
HEAD_DIM = 256
Q_TILE = 256
K_TILE = 256
HEADS_PER_STEP = 2


def rms_norm(x_f32, gain_f32):
    mean_sq = jnp.mean(x_f32 * x_f32, axis=-1, keepdims=True)
    return (x_f32 * lax.rsqrt(mean_sq + NORM_EPS) * (1.0 + gain_f32)).astype(jnp.bfloat16)


def rotate(vals, cos2, sin2):
    low = vals[:, :128]
    swapped = jnp.concatenate([low[:, 64:], low[:, :64]], axis=1)
    return jnp.concatenate([low * cos2 + swapped * sin2, vals[:, 128:]], axis=1)


def nt_dot(a, b):
    return lax.dot_general(a, b, (((1,), (1,)), ((), ())), preferred_element_type=jnp.float32)


def nn_dot(a, b):
    return lax.dot_general(a, b, (((1,), (0,)), ((), ())), preferred_element_type=jnp.float32)


def attention_kernel(first_blk, q_ref, do_ref, k_ref, v_ref, low_ref, cos_ref, sin_ref,
                     o_ref, dq_ref, dkv_ref,
                     cap, s_scr, dp_scr, q2, do2, q2t, do2t, m_acc, l_acc, d_acc, o_acc, dq_acc, dk_t, dv_t):
    q_idx, h_idx = pl.program_id(0), pl.program_id(1)
    rows = HEADS_PER_STEP * Q_TILE
    scale = HEAD_DIM ** -0.5
    kb_low = first_blk[q_idx]
    kb_end = q_idx + WINDOW // K_TILE + 1

    @pl.when(jnp.logical_and(q_idx == 0, h_idx == 0))
    def _():
        dk_t[...] = jnp.zeros_like(dk_t)
        dv_t[...] = jnp.zeros_like(dv_t)

    @pl.when(h_idx == 0)
    def _():
        q_pos = WINDOW + q_idx * Q_TILE + lax.broadcasted_iota(jnp.int32, (Q_TILE, K_TILE), 0)
        low = low_ref[...]

        def fill(kb, _):
            k_pos = kb * K_TILE + lax.broadcasted_iota(jnp.int32, (Q_TILE, K_TILE), 1)
            allowed = jnp.logical_and(k_pos >= low, k_pos <= q_pos)
            cap[kb - q_idx] = jnp.where(allowed, jnp.inf, NEG_BIG)
            return 0

        lax.fori_loop(kb_low, kb_end, fill, 0)

    for h in range(HEADS_PER_STEP):
        cols = slice(h * HEAD_DIM, (h + 1) * HEAD_DIM)
        span = slice(h * Q_TILE, (h + 1) * Q_TILE)
        low_half = q_ref[:, h * HEAD_DIM:h * HEAD_DIM + 128]
        turned = low_half * cos_ref[...] + pltpu.roll(low_half, 64, 1) * sin_ref[...]
        q2[span, :128] = (turned * scale).astype(jnp.bfloat16)
        q2[span, 128:] = (q_ref[:, h * HEAD_DIM + 128:(h + 1) * HEAD_DIM] * scale).astype(jnp.bfloat16)
        do2[span, :] = do_ref[:, cols]
    q2t[...] = q2[...].T
    do2t[...] = do2[...].T

    m_acc[...] = jnp.full_like(m_acc, NEG_BIG)

    def scores(kb, _):
        keys = k_ref[pl.ds(pl.multiple_of(kb * K_TILE, K_TILE), K_TILE), :]
        s = nt_dot(q2[...], keys)
        slot = kb - q_idx
        s = jnp.minimum(s.reshape(HEADS_PER_STEP, Q_TILE, K_TILE), cap[slot][None]).reshape(rows, K_TILE)
        s_scr[slot] = s
        m_acc[...] = jnp.maximum(m_acc[...], jnp.maximum(s[:, :128], s[:, 128:]))
        return 0

    lax.fori_loop(kb_low, kb_end, scores, 0)
    row_max = jnp.max(m_acc[...], axis=1, keepdims=True)
    m_acc[...] = jnp.broadcast_to(row_max, m_acc.shape)
    l_acc[...] = jnp.zeros_like(l_acc)
    d_acc[...] = jnp.zeros_like(d_acc)

    def exps(kb, _):
        vals = v_ref[pl.ds(pl.multiple_of(kb * K_TILE, K_TILE), K_TILE), :]
        slot = kb - q_idx
        dp = nt_dot(do2[...], vals)
        m = m_acc[...]
        e0 = jnp.exp(s_scr[slot, :, :128] - m)
        e1 = jnp.exp(s_scr[slot, :, 128:] - m)
        s_scr[slot, :, :128] = e0
        s_scr[slot, :, 128:] = e1
        dp_scr[slot] = dp
        l_acc[...] += e0 + e1
        d_acc[...] += e0 * dp[:, :128] + e1 * dp[:, 128:]
        return 0

    lax.fori_loop(kb_low, kb_end, exps, 0)
    inv_l = 1.0 / jnp.sum(l_acc[...], axis=1, keepdims=True)
    delta = jnp.sum(d_acc[...], axis=1, keepdims=True) * inv_l
    l_acc[...] = jnp.broadcast_to(inv_l, l_acc.shape)
    d_acc[...] = jnp.broadcast_to(delta, d_acc.shape)
    o_acc[...] = jnp.zeros_like(o_acc)
    dq_acc[...] = jnp.zeros_like(dq_acc)

    def grads(kb, _):
        start = pl.multiple_of(kb * K_TILE, K_TILE)
        keys = k_ref[pl.ds(start, K_TILE), :]
        vals = v_ref[pl.ds(start, K_TILE), :]
        slot = kb - q_idx
        inv = jnp.concatenate([l_acc[...], l_acc[...]], axis=1)
        dlt = jnp.concatenate([d_acc[...], d_acc[...]], axis=1)
        p = s_scr[slot] * inv
        ds = (p * (dp_scr[slot] - dlt)).astype(jnp.bfloat16)
        pb = p.astype(jnp.bfloat16)
        o_acc[...] += nn_dot(pb, vals)
        dq_acc[...] += nn_dot(ds, keys)
        dk_t[kb] += nn_dot(q2t[...], ds)
        dv_t[kb] += nn_dot(do2t[...], pb)
        return 0

    lax.fori_loop(kb_low, kb_end, grads, 0)

    for h in range(HEADS_PER_STEP):
        span = slice(h * Q_TILE, (h + 1) * Q_TILE)
        o_ref[:, h * HEAD_DIM:(h + 1) * HEAD_DIM] = o_acc[span, :].astype(jnp.bfloat16)
        dq = dq_acc[span, :].astype(jnp.bfloat16).astype(jnp.float32)
        low_half = dq[:, :128]
        turned = low_half * cos_ref[...] - pltpu.roll(low_half, 64, 1) * sin_ref[...]
        dq_ref[:, h * HEAD_DIM:h * HEAD_DIM + 128] = (turned * scale).astype(jnp.bfloat16)
        dq_ref[:, h * HEAD_DIM + 128:(h + 1) * HEAD_DIM] = (dq[:, 128:] * scale).astype(jnp.bfloat16)

    @pl.when(jnp.logical_and(q_idx == pl.num_programs(0) - 1, h_idx == pl.num_programs(1) - 1))
    def _():
        def flush(kb, _):
            start = pl.multiple_of(kb * K_TILE, K_TILE)
            dkv_ref[pl.ds(start, K_TILE), :HEAD_DIM] = dk_t[kb].T
            dkv_ref[pl.ds(start, K_TILE), HEAD_DIM:] = dv_t[kb].T
            return 0

        lax.fori_loop(0, dk_t.shape[0], flush, 0)


def attention(q_lin, d_o, k_ext, v_ext, low, cos2, sin2):
    tokens, width = q_lin.shape
    span = k_ext.shape[0]
    n_q = tokens // Q_TILE
    step_cols = HEADS_PER_STEP * HEAD_DIM
    rows = HEADS_PER_STEP * Q_TILE
    slots = WINDOW // K_TILE + 1
    first_blk = low[::Q_TILE, 0] // K_TILE
    tile = pl.BlockSpec((Q_TILE, step_cols), lambda i, h, fb: (i, h))
    full = pl.BlockSpec((span, HEAD_DIM), lambda i, h, fb: (0, 0))
    side = pl.BlockSpec((Q_TILE, 128), lambda i, h, fb: (i, 0))
    pairs = tokens * width // HEAD_DIM * WINDOW
    f32 = jnp.float32
    return pl.pallas_call(
        attention_kernel,
        out_shape=(jax.ShapeDtypeStruct((tokens, width), jnp.bfloat16),
                   jax.ShapeDtypeStruct((tokens, width), jnp.bfloat16),
                   jax.ShapeDtypeStruct((span, 2 * HEAD_DIM), f32)),
        grid_spec=pltpu.PrefetchScalarGridSpec(
            num_scalar_prefetch=1,
            grid=(n_q, width // step_cols),
            in_specs=[tile, tile, full, full, pl.BlockSpec((Q_TILE, 1), lambda i, h, fb: (i, 0)), side, side],
            out_specs=[tile, tile, pl.BlockSpec((span, 2 * HEAD_DIM), lambda i, h, fb: (0, 0))],
            scratch_shapes=[
                pltpu.VMEM((slots, Q_TILE, K_TILE), f32),
                pltpu.VMEM((slots, rows, K_TILE), f32),
                pltpu.VMEM((slots, rows, K_TILE), f32),
                pltpu.VMEM((rows, HEAD_DIM), jnp.bfloat16),
                pltpu.VMEM((rows, HEAD_DIM), jnp.bfloat16),
                pltpu.VMEM((HEAD_DIM, rows), jnp.bfloat16),
                pltpu.VMEM((HEAD_DIM, rows), jnp.bfloat16),
                pltpu.VMEM((rows, 128), f32),
                pltpu.VMEM((rows, 128), f32),
                pltpu.VMEM((rows, 128), f32),
                pltpu.VMEM((rows, HEAD_DIM), f32),
                pltpu.VMEM((rows, HEAD_DIM), f32),
                pltpu.VMEM((span // K_TILE, HEAD_DIM, K_TILE), f32),
                pltpu.VMEM((span // K_TILE, HEAD_DIM, K_TILE), f32),
            ]),
        compiler_params=pltpu.CompilerParams(
            dimension_semantics=("arbitrary", "arbitrary"), vmem_limit_bytes=60 * 1024 * 1024),
        cost_estimate=pl.CostEstimate(flops=12 * pairs * HEAD_DIM, bytes_accessed=32 * 1024 * 1024, transcendentals=pairs),
    )(first_blk, q_lin, d_o, k_ext, v_ext, low, cos2, sin2)


def solution(mesh):
    row_spec = P("dp", "sp", None)
    tok_spec = P("dp", "sp")
    mat_spec = P(None, None)
    grad_mat = P("dp", None)
    n_sp = mesh.shape["sp"]
    f32, bf16 = jnp.float32, jnp.bfloat16

    def tn_dot(a, b):
        return lax.dot_general(a, b, (((0,), (0,)), ((), ())), preferred_element_type=f32).astype(bf16)

    def gather(a):
        return lax.all_gather(a, "sp", axis=0, tiled=True)

    def put(buf, part, row):
        return lax.dynamic_update_slice(buf, part, (row, 0))

    def step(x, seg_ids, positions, out_grad, norm_scale, w_q, w_k, w_v, w_o, b_o):
        tokens, width = x.shape[1], x.shape[2]
        heads_width = w_q.shape[1]
        back = WINDOW // tokens
        me = lax.axis_index("sp")
        og = out_grad[0]
        og_all = gather(og)

        x_f32 = x[0].astype(f32)
        normed, norm_pull = jax.vjp(rms_norm, x_f32, norm_scale.astype(f32))
        half = HEAD_DIM // 4
        inv_freq = ROPE_BASE ** (-(jnp.arange(half, dtype=f32) * 2.0 / (HEAD_DIM // 2)))
        angles = positions[0].astype(f32)[:, None] * inv_freq
        cos_a, sin_a = jnp.cos(angles), jnp.sin(angles)
        cos2 = jnp.concatenate([cos_a, cos_a], axis=1)
        sin2 = jnp.concatenate([-sin_a, sin_a], axis=1)

        keys = rotate(nn_dot(normed, w_k), cos2, sin2).astype(bf16)
        values = nn_dot(normed, w_v).astype(bf16)
        kv = jnp.concatenate([keys, values], axis=1)

        def shift(a, dist):
            return lax.ppermute(a, "sp", [(i, i + dist) for i in range(n_sp - dist)])

        kv_ext = jnp.concatenate([shift(kv, d) for d in range(back, 0, -1)] + [kv], axis=0)
        seg = seg_ids[0]
        seg_ext = jnp.concatenate([shift(seg, d) for d in range(back, 0, -1)] + [seg])
        ext_idx = jnp.arange(seg_ext.shape[0])
        before = (seg_ext[None, :] < seg[:, None]) | (ext_idx < (back - me) * tokens)[None, :]
        doc_low = jnp.sum(before.astype(jnp.int32), axis=1)
        low = jnp.maximum(doc_low, jnp.arange(tokens) + 1).astype(jnp.int32)[:, None]

        blanks = [jnp.zeros(shape, bf16) for shape in
                  ((heads_width, width), (width, heads_width), (width, HEAD_DIM), (width, HEAD_DIM))]
        *blanks, low = lax.optimization_barrier((*blanks, low))
        d_o = nt_dot(og, w_o).astype(bf16)
        q_lin = nn_dot(normed, w_q)
        o_tok, dq_lin, dkv_ext = attention(q_lin, d_o, kv_ext[:, :HEAD_DIM], kv_ext[:, HEAD_DIM:], low, cos2, sin2)

        n_cut = width // 4
        o_cut = heads_width // 2
        n_first = gather(normed[:, :n_cut])
        late_normed, _ = lax.optimization_barrier((normed, o_tok))
        o_a = gather(o_tok[:, :o_cut])
        o_b = gather(o_tok[:, o_cut:])

        block_out = (x_f32 + nn_dot(o_tok, w_o) + b_o.astype(f32)).astype(bf16)

        dkv = dkv_ext[back * tokens:]
        for d in range(1, back + 1):
            part = dkv_ext[(back - d) * tokens:(back - d + 1) * tokens]
            dkv = dkv + lax.ppermute(part, "sp", [(i, i - d) for i in range(d, n_sp)])
        dkv = dkv.astype(bf16)
        dk_lin = rotate(dkv[:, :HEAD_DIM].astype(f32), cos2, -sin2).astype(bf16)
        dv_lin = dkv[:, HEAD_DIM:]
        dkv_lin = jnp.concatenate([dk_lin, dv_lin], axis=1)

        dq_all = gather(dq_lin)
        dkv_all = gather(dkv_lin)
        d_normed = (nt_dot(dq_lin, w_q) + nt_dot(dk_lin, w_k) + nt_dot(dv_lin, w_v)).astype(bf16)
        dx_norm, gain_part = norm_pull(d_normed)
        x_grad = (og.astype(f32) + dx_norm).astype(bf16)
        small = jnp.stack([gain_part, jnp.sum(og, axis=0, dtype=f32)])
        hop = 1
        while hop < n_sp:
            small = small + lax.ppermute(small, "sp", [(i, i ^ hop) for i in range(n_sp)])
            hop *= 2
        small = small.astype(bf16)

        n_cuts = [n_first] + [gather(late_normed[:, c * n_cut:(c + 1) * n_cut]) for c in range(1, 4)]
        w_o_grad, w_q_grad, w_k_grad, w_v_grad = blanks
        for c, o_c in enumerate((o_a, o_b)):
            w_o_grad = put(w_o_grad, tn_dot(o_c, og_all), c * o_cut)
        for c, n_c in enumerate(n_cuts):
            w_q_grad = put(w_q_grad, tn_dot(n_c, dq_all), c * n_cut)
            w_kv = tn_dot(n_c, dkv_all)
            w_k_grad = put(w_k_grad, w_kv[:, :HEAD_DIM], c * n_cut)
            w_v_grad = put(w_v_grad, w_kv[:, HEAD_DIM:], c * n_cut)
        return (block_out[None], x_grad[None], small[0], w_q_grad, w_k_grad, w_v_grad,
                w_o_grad, small[1])

    return jax.shard_map(step, mesh=mesh,
                         in_specs=(row_spec, tok_spec, tok_spec, row_spec, P(None), mat_spec, mat_spec, mat_spec, mat_spec, P(None)),
                         out_specs=(row_spec, row_spec, P("dp"), grad_mat, grad_mat, grad_mat, grad_mat, P("dp")),
                         check_vma=False)
```

```python
import jax
import jax.numpy as jnp
from jax import lax
from jax.experimental import pallas as pl
from jax.experimental.pallas import tpu as pltpu
from jax.sharding import PartitionSpec as P


WINDOW = 2048
NORM_EPS = 1e-6
ROPE_BASE = 10000.0
NEG_BIG = -1e30
HEAD_DIM = 256
Q_TILE = 256
K_TILE = 256
HEADS_PER_STEP = 2


def rms_norm(x_f32, gain_f32):
    mean_sq = jnp.mean(x_f32 * x_f32, axis=-1, keepdims=True)
    return (x_f32 * lax.rsqrt(mean_sq + NORM_EPS) * (1.0 + gain_f32)).astype(jnp.bfloat16)


def rotate(vals, cos2, sin2):
    low = vals[:, :128]
    swapped = jnp.concatenate([low[:, 64:], low[:, :64]], axis=1)
    return jnp.concatenate([low * cos2 + swapped * sin2, vals[:, 128:]], axis=1)


def nt_dot(a, b):
    return lax.dot_general(a, b, (((1,), (1,)), ((), ())), preferred_element_type=jnp.float32)


def nn_dot(a, b):
    return lax.dot_general(a, b, (((1,), (0,)), ((), ())), preferred_element_type=jnp.float32)


def attention_kernel(first_blk, base_blk, q_ref, do_ref, k_ref, v_ref, low_ref, cos_ref, sin_ref,
                     o_ref, dq_ref, dkv_ref,
                     cap, s_scr, dp_scr, q2, do2, q2t, do2t, m_acc, l_acc, d_acc, o_acc, dq_acc, dk_t, dv_t):
    q_idx, h_idx = pl.program_id(0), pl.program_id(1)
    rows = HEADS_PER_STEP * Q_TILE
    scale = HEAD_DIM ** -0.5
    kb_low = first_blk[q_idx]
    kb_end = q_idx + WINDOW // K_TILE + 1
    base = base_blk[0]

    @pl.when(jnp.logical_and(q_idx == 0, h_idx == 0))
    def _():
        dk_t[...] = jnp.zeros_like(dk_t)
        dv_t[...] = jnp.zeros_like(dv_t)

    @pl.when(h_idx == 0)
    def _():
        q_pos = WINDOW + q_idx * Q_TILE + lax.broadcasted_iota(jnp.int32, (Q_TILE, K_TILE), 0)
        low = low_ref[...]

        def fill(kb, _):
            k_pos = kb * K_TILE + lax.broadcasted_iota(jnp.int32, (Q_TILE, K_TILE), 1)
            allowed = jnp.logical_and(k_pos >= low, k_pos <= q_pos)
            cap[kb - q_idx] = jnp.where(allowed, jnp.inf, NEG_BIG)
            return 0

        lax.fori_loop(kb_low, kb_end, fill, 0)

    for h in range(HEADS_PER_STEP):
        cols = slice(h * HEAD_DIM, (h + 1) * HEAD_DIM)
        span = slice(h * Q_TILE, (h + 1) * Q_TILE)
        low_half = q_ref[:, h * HEAD_DIM:h * HEAD_DIM + 128]
        turned = low_half * cos_ref[...] + pltpu.roll(low_half, 64, 1) * sin_ref[...]
        q2[span, :128] = (turned * scale).astype(jnp.bfloat16)
        q2[span, 128:] = (q_ref[:, h * HEAD_DIM + 128:(h + 1) * HEAD_DIM] * scale).astype(jnp.bfloat16)
        do2[span, :] = do_ref[:, cols]
    q2t[...] = q2[...].T
    do2t[...] = do2[...].T

    m_acc[...] = jnp.full_like(m_acc, NEG_BIG)

    def scores(kb, _):
        keys = k_ref[pl.ds(pl.multiple_of((kb + base) * K_TILE, K_TILE), K_TILE), :]
        s = nt_dot(q2[...], keys)
        slot = kb - q_idx
        s = jnp.minimum(s.reshape(HEADS_PER_STEP, Q_TILE, K_TILE), cap[slot][None]).reshape(rows, K_TILE)
        s_scr[slot] = s
        m_acc[...] = jnp.maximum(m_acc[...], jnp.maximum(s[:, :128], s[:, 128:]))
        return 0

    lax.fori_loop(kb_low, kb_end, scores, 0)
    row_max = jnp.max(m_acc[...], axis=1, keepdims=True)
    m_acc[...] = jnp.broadcast_to(row_max, m_acc.shape)
    l_acc[...] = jnp.zeros_like(l_acc)
    d_acc[...] = jnp.zeros_like(d_acc)

    def exps(kb, _):
        vals = v_ref[pl.ds(pl.multiple_of((kb + base) * K_TILE, K_TILE), K_TILE), :]
        slot = kb - q_idx
        dp = nt_dot(do2[...], vals)
        m = m_acc[...]
        e0 = jnp.exp(s_scr[slot, :, :128] - m)
        e1 = jnp.exp(s_scr[slot, :, 128:] - m)
        s_scr[slot, :, :128] = e0
        s_scr[slot, :, 128:] = e1
        dp_scr[slot] = dp
        l_acc[...] += e0 + e1
        d_acc[...] += e0 * dp[:, :128] + e1 * dp[:, 128:]
        return 0

    lax.fori_loop(kb_low, kb_end, exps, 0)
    inv_l = 1.0 / jnp.sum(l_acc[...], axis=1, keepdims=True)
    delta = jnp.sum(d_acc[...], axis=1, keepdims=True) * inv_l
    l_acc[...] = jnp.broadcast_to(inv_l, l_acc.shape)
    d_acc[...] = jnp.broadcast_to(delta, d_acc.shape)
    o_acc[...] = jnp.zeros_like(o_acc)
    dq_acc[...] = jnp.zeros_like(dq_acc)

    def grads(kb, _):
        start = pl.multiple_of((kb + base) * K_TILE, K_TILE)
        keys = k_ref[pl.ds(start, K_TILE), :]
        vals = v_ref[pl.ds(start, K_TILE), :]
        slot = kb - q_idx
        inv = jnp.concatenate([l_acc[...], l_acc[...]], axis=1)
        dlt = jnp.concatenate([d_acc[...], d_acc[...]], axis=1)
        p = s_scr[slot] * inv
        ds = (p * (dp_scr[slot] - dlt)).astype(jnp.bfloat16)
        pb = p.astype(jnp.bfloat16)
        o_acc[...] += nn_dot(pb, vals)
        dq_acc[...] += nn_dot(ds, keys)
        dk_t[kb] += nn_dot(q2t[...], ds)
        dv_t[kb] += nn_dot(do2t[...], pb)
        return 0

    lax.fori_loop(kb_low, kb_end, grads, 0)

    for h in range(HEADS_PER_STEP):
        span = slice(h * Q_TILE, (h + 1) * Q_TILE)
        o_ref[:, h * HEAD_DIM:(h + 1) * HEAD_DIM] = o_acc[span, :].astype(jnp.bfloat16)
        dq = dq_acc[span, :].astype(jnp.bfloat16).astype(jnp.float32)
        low_half = dq[:, :128]
        turned = low_half * cos_ref[...] - pltpu.roll(low_half, 64, 1) * sin_ref[...]
        dq_ref[:, h * HEAD_DIM:h * HEAD_DIM + 128] = (turned * scale).astype(jnp.bfloat16)
        dq_ref[:, h * HEAD_DIM + 128:(h + 1) * HEAD_DIM] = (dq[:, 128:] * scale).astype(jnp.bfloat16)

    @pl.when(jnp.logical_and(q_idx == pl.num_programs(0) - 1, h_idx == pl.num_programs(1) - 1))
    def _():
        def flush(blk, _):
            rows_out = pl.ds(pl.multiple_of(blk * K_TILE, K_TILE), K_TILE)
            kb = blk - base
            inside = jnp.logical_and(kb >= 0, kb < dk_t.shape[0])

            @pl.when(inside)
            def _():
                dkv_ref[rows_out, :HEAD_DIM] = dk_t[kb].T
                dkv_ref[rows_out, HEAD_DIM:] = dv_t[kb].T

            @pl.when(jnp.logical_not(inside))
            def _():
                dkv_ref[rows_out, :] = jnp.zeros((K_TILE, 2 * HEAD_DIM), jnp.float32)

            return 0

        lax.fori_loop(0, dkv_ref.shape[0] // K_TILE, flush, 0)


def attention(q_lin, d_o, kv_all, low, base_blk, cos2, sin2):
    tokens, width = q_lin.shape
    span = kv_all.shape[0]
    n_q = tokens // Q_TILE
    step_cols = HEADS_PER_STEP * HEAD_DIM
    rows = HEADS_PER_STEP * Q_TILE
    slots = WINDOW // K_TILE + 1
    first_blk = low[::Q_TILE, 0] // K_TILE
    tile = pl.BlockSpec((Q_TILE, step_cols), lambda i, h, fb, bb: (i, h))
    k_spec = pl.BlockSpec((span, HEAD_DIM), lambda i, h, fb, bb: (0, 0))
    v_spec = pl.BlockSpec((span, HEAD_DIM), lambda i, h, fb, bb: (0, 1))
    local_blks = (WINDOW + tokens) // K_TILE
    side = pl.BlockSpec((Q_TILE, 128), lambda i, h, fb, bb: (i, 0))
    pairs = tokens * width // HEAD_DIM * WINDOW
    f32 = jnp.float32
    return pl.pallas_call(
        attention_kernel,
        out_shape=(jax.ShapeDtypeStruct((tokens, width), jnp.bfloat16),
                   jax.ShapeDtypeStruct((tokens, width), jnp.bfloat16),
                   jax.ShapeDtypeStruct((span, 2 * HEAD_DIM), f32)),
        grid_spec=pltpu.PrefetchScalarGridSpec(
            num_scalar_prefetch=2,
            grid=(n_q, width // step_cols),
            in_specs=[tile, tile, k_spec, v_spec, pl.BlockSpec((Q_TILE, 1), lambda i, h, fb, bb: (i, 0)), side, side],
            out_specs=[tile, tile, pl.BlockSpec((span, 2 * HEAD_DIM), lambda i, h, fb, bb: (0, 0))],
            scratch_shapes=[
                pltpu.VMEM((slots, Q_TILE, K_TILE), f32),
                pltpu.VMEM((slots, rows, K_TILE), f32),
                pltpu.VMEM((slots, rows, K_TILE), f32),
                pltpu.VMEM((rows, HEAD_DIM), jnp.bfloat16),
                pltpu.VMEM((rows, HEAD_DIM), jnp.bfloat16),
                pltpu.VMEM((HEAD_DIM, rows), jnp.bfloat16),
                pltpu.VMEM((HEAD_DIM, rows), jnp.bfloat16),
                pltpu.VMEM((rows, 128), f32),
                pltpu.VMEM((rows, 128), f32),
                pltpu.VMEM((rows, 128), f32),
                pltpu.VMEM((rows, HEAD_DIM), f32),
                pltpu.VMEM((rows, HEAD_DIM), f32),
                pltpu.VMEM((local_blks, HEAD_DIM, K_TILE), f32),
                pltpu.VMEM((local_blks, HEAD_DIM, K_TILE), f32),
            ]),
        compiler_params=pltpu.CompilerParams(
            dimension_semantics=("arbitrary", "arbitrary"), vmem_limit_bytes=60 * 1024 * 1024),
        cost_estimate=pl.CostEstimate(flops=12 * pairs * HEAD_DIM, bytes_accessed=32 * 1024 * 1024, transcendentals=pairs),
    )(first_blk, base_blk, q_lin, d_o, kv_all, kv_all, low, cos2, sin2)


def solution(mesh):
    row_spec = P("dp", "sp", None)
    tok_spec = P("dp", "sp")
    mat_spec = P(None, None)
    grad_mat = P("dp", None)
    n_sp = mesh.shape["sp"]
    f32, bf16 = jnp.float32, jnp.bfloat16

    def tn_dot(a, b):
        return lax.dot_general(a, b, (((0,), (0,)), ((), ())), preferred_element_type=f32).astype(bf16)

    def gather(a):
        return lax.all_gather(a, "sp", axis=0, tiled=True)

    def gather_chips(a):
        groups = [list(range(core, n_sp, 2)) for core in (0, 1)]
        return lax.all_gather(a, "sp", axis=0, tiled=True, axis_index_groups=groups)

    def swap(a, bit):
        return lax.ppermute(a, "sp", [(i, i ^ bit) for i in range(n_sp)])

    def tree_gather(a, me):
        rows = a.shape[0]
        half = rows // 2
        a_x, a_y, a_c = swap(a, 2), swap(a, 4), swap(a, 1)
        far = jnp.concatenate([swap(a_y[:half], 2), swap(a_x[half:], 4)], axis=0)
        mine = {0: a, 2: a_x, 4: a_y, 6: far}
        other = {0: a_c, 2: swap(a_x, 1), 4: swap(a_y, 1), 6: swap(far, 1)}
        out = jnp.zeros((n_sp * rows,) + a.shape[1:], a.dtype)
        for m, shard in mine.items():
            for bit, part in ((m, shard), (m ^ 1, other[m])):
                out = lax.dynamic_update_slice(out, part, ((me ^ bit) * rows,) + (0,) * (a.ndim - 1))
        return out

    def pair(core, own, got):
        out = jnp.zeros((2,) + own.shape, own.dtype)
        return put(put(out, own, core, 0), got, 1 - core, 0)

    def trade_halves(a, core):
        rows, half = a.shape[0], a.shape[1] // 2
        first, second = a[:, :half], a[:, half:]
        keep = jnp.where(core == 0, first, second)
        got = swap(jnp.where(core == 0, second, first), 1)
        return pair(core, keep, got).reshape(2 * rows, half)

    def tree_scatter_sum(a, me):
        rows = a.shape[0] // n_sp
        core, x_bit, y_bit = me & 1, (me >> 1) & 1, (me >> 2) & 1
        parts = a.reshape(n_sp // 2, 2, rows, a.shape[1])

        def pick(arr, idx, axis):
            return lax.dynamic_index_in_dim(arr, idx, axis, keepdims=False)

        got = swap(pick(parts, 1 - core, 1), 1)
        parts = pick(parts, core, 1) + got
        parts = parts.reshape(2, 2, rows, a.shape[1])
        half = rows // 2
        top, low = parts[:, :, :half], parts[:, :, half:]
        top = pick(top, x_bit, 1) + swap(pick(top, 1 - x_bit, 1), 2)
        low = pick(low, y_bit, 0) + swap(pick(low, 1 - y_bit, 0), 4)
        top = pick(top, y_bit, 0) + swap(pick(top, 1 - y_bit, 0), 4)
        low = pick(low, x_bit, 0) + swap(pick(low, 1 - x_bit, 0), 2)
        return jnp.concatenate([top, low], axis=0)

    def put(buf, part, core, col):
        return lax.dynamic_update_slice(buf, part[None], (core, 0, col))

    def step(x, seg_ids, positions, out_grad, norm_scale, w_q, w_k, w_v, w_o, b_o):
        tokens, width = x.shape[1], x.shape[2]
        heads_width = w_q.shape[1]
        me = lax.axis_index("sp")
        core = me & 1
        og = out_grad[0]
        og_all = gather(og)
        seg = seg_ids[0]
        seg_all = tree_gather(seg, me)

        x_f32 = x[0].astype(f32)
        normed, norm_pull = jax.vjp(rms_norm, x_f32, norm_scale.astype(f32))
        half = HEAD_DIM // 4
        inv_freq = ROPE_BASE ** (-(jnp.arange(half, dtype=f32) * 2.0 / (HEAD_DIM // 2)))
        angles = positions[0].astype(f32)[:, None] * inv_freq
        cos_a, sin_a = jnp.cos(angles), jnp.sin(angles)
        cos2 = jnp.concatenate([cos_a, cos_a], axis=1)
        sin2 = jnp.concatenate([-sin_a, sin_a], axis=1)

        keys = rotate(nn_dot(normed, w_k), cos2, sin2).astype(bf16)
        values = nn_dot(normed, w_v).astype(bf16)
        n_half = gather_chips(trade_halves(normed, core))
        kv_all = tree_gather(jnp.concatenate([keys, values], axis=1), me)

        base = me * tokens - WINDOW
        doc_start = jnp.sum((seg_all[None, :] < seg[:, None]).astype(jnp.int32), axis=1)
        low = jnp.maximum(doc_start - base, jnp.arange(tokens) + 1).astype(jnp.int32)[:, None]
        base_blk = (base // K_TILE).astype(jnp.int32).reshape(1)

        blanks = [jnp.ones(shape, bf16) for shape in ((2, heads_width // 2, width), (2, width // 2, heads_width))]
        *blanks, low = lax.optimization_barrier((*blanks, low))
        d_o = nt_dot(og, w_o).astype(bf16)
        q_lin = nn_dot(normed, w_q)
        o_tok, dq_lin, dkv_part = attention(q_lin, d_o, kv_all, low, base_blk, cos2, sin2)

        o_half = gather_chips(trade_halves(o_tok, core))
        cut = heads_width * 3 // 4
        dq_a = gather(dq_lin[:, :cut])
        dq_b = gather(dq_lin[:, cut:])

        block_out = (x_f32 + nn_dot(o_tok, w_o) + b_o.astype(f32)).astype(bf16)

        dkv = tree_scatter_sum(dkv_part, me).astype(bf16)
        dk_lin = rotate(dkv[:, :HEAD_DIM].astype(f32), cos2, -sin2).astype(bf16)
        dv_lin = dkv[:, HEAD_DIM:]
        dkv_all = tree_gather(jnp.concatenate([dk_lin, dv_lin], axis=1), me)

        d_normed = (nt_dot(dq_lin, w_q) + nt_dot(dk_lin, w_k) + nt_dot(dv_lin, w_v)).astype(bf16)
        dx_norm, gain_part = norm_pull(d_normed)
        x_grad = (og.astype(f32) + dx_norm).astype(bf16)
        small = jnp.stack([gain_part, jnp.sum(og, axis=0, dtype=f32)])
        for bit in (1, 2, 4):
            got = swap(small, bit)
            small = small + got
        small = small.astype(bf16)

        w_o_grad, w_q_grad = blanks

        def both(buf, part, col):
            got = swap(part, 1)
            return put(put(buf, part, core, col), got, 1 - core, col)

        o_rows = lax.optimization_barrier(tn_dot(o_half, og_all))
        w_o_grad = both(w_o_grad, o_rows, 0).reshape(heads_width, width)
        kv_rows = lax.optimization_barrier(tn_dot(n_half, dkv_all))
        w_kv_grad = pair(core, kv_rows, swap(kv_rows, 1)).reshape(width, 2 * HEAD_DIM)
        w_k_grad, w_v_grad = w_kv_grad[:, :HEAD_DIM], w_kv_grad[:, HEAD_DIM:]
        qa_rows = tn_dot(n_half, dq_a)
        w_q_grad = both(w_q_grad, qa_rows, 0)
        qb_rows = tn_dot(n_half, dq_b)
        w_q_grad = both(w_q_grad, qb_rows, cut).reshape(width, heads_width)
        return (block_out[None], x_grad[None], small[0], w_q_grad, w_k_grad, w_v_grad, w_o_grad, small[1])

    return jax.shard_map(step, mesh=mesh,
                         in_specs=(row_spec, tok_spec, tok_spec, row_spec, P(None), mat_spec, mat_spec, mat_spec, mat_spec, P(None)),
                         out_specs=(row_spec, row_spec, P("dp"), grad_mat, grad_mat, grad_mat, grad_mat, P("dp")),
                         check_vma=False)
```

```python
import jax
import jax.numpy as jnp
from jax import lax
from jax.experimental import pallas as pl
from jax.experimental.pallas import tpu as pltpu
from jax.sharding import PartitionSpec as P


WINDOW = 2048
NORM_EPS = 1e-6
ROPE_BASE = 10000.0
NEG_BIG = -1e30
HEAD_DIM = 256
Q_TILE = 256
K_TILE = 256
HEADS_PER_STEP = 2


def rms_norm(x_f32, gain_f32):
    mean_sq = jnp.mean(x_f32 * x_f32, axis=-1, keepdims=True)
    return (x_f32 * lax.rsqrt(mean_sq + NORM_EPS) * (1.0 + gain_f32)).astype(jnp.bfloat16)


def rotate(vals, cos2, sin2):
    low = vals[:, :128]
    swapped = jnp.concatenate([low[:, 64:], low[:, :64]], axis=1)
    return jnp.concatenate([low * cos2 + swapped * sin2, vals[:, 128:]], axis=1)


def nt_dot(a, b):
    return lax.dot_general(a, b, (((1,), (1,)), ((), ())), preferred_element_type=jnp.float32)


def nn_dot(a, b):
    return lax.dot_general(a, b, (((1,), (0,)), ((), ())), preferred_element_type=jnp.float32)


def attention_kernel(first_blk, base_blk, q_ref, do_ref, k_ref, v_ref, low_ref, cos_ref, sin_ref,
                     o_ref, dq_ref, dkv_ref,
                     cap, s_scr, dp_scr, q2, do2, q2t, do2t, m_acc, l_acc, d_acc, o_acc, dq_acc, dk_t, dv_t):
    q_idx, h_idx = pl.program_id(0), pl.program_id(1)
    rows = HEADS_PER_STEP * Q_TILE
    scale = HEAD_DIM ** -0.5
    kb_low = first_blk[q_idx]
    kb_end = q_idx + WINDOW // K_TILE + 1
    base = base_blk[0]

    @pl.when(jnp.logical_and(q_idx == 0, h_idx == 0))
    def _():
        dk_t[...] = jnp.zeros_like(dk_t)
        dv_t[...] = jnp.zeros_like(dv_t)

    @pl.when(h_idx == 0)
    def _():
        q_pos = WINDOW + q_idx * Q_TILE + lax.broadcasted_iota(jnp.int32, (Q_TILE, K_TILE), 0)
        low = low_ref[...]

        def fill(kb, _):
            k_pos = kb * K_TILE + lax.broadcasted_iota(jnp.int32, (Q_TILE, K_TILE), 1)
            allowed = jnp.logical_and(k_pos >= low, k_pos <= q_pos)
            cap[kb - q_idx] = jnp.where(allowed, jnp.inf, NEG_BIG)
            return 0

        lax.fori_loop(kb_low, kb_end, fill, 0)

    for h in range(HEADS_PER_STEP):
        cols = slice(h * HEAD_DIM, (h + 1) * HEAD_DIM)
        span = slice(h * Q_TILE, (h + 1) * Q_TILE)
        low_half = q_ref[:, h * HEAD_DIM:h * HEAD_DIM + 128]
        turned = low_half * cos_ref[...] + pltpu.roll(low_half, 64, 1) * sin_ref[...]
        q2[span, :128] = (turned * scale).astype(jnp.bfloat16)
        q2[span, 128:] = (q_ref[:, h * HEAD_DIM + 128:(h + 1) * HEAD_DIM] * scale).astype(jnp.bfloat16)
        do2[span, :] = do_ref[:, cols]
    q2t[...] = q2[...].T
    do2t[...] = do2[...].T

    m_acc[...] = jnp.full_like(m_acc, NEG_BIG)

    def scores(kb, _):
        keys = k_ref[pl.ds(pl.multiple_of((kb + base) * K_TILE, K_TILE), K_TILE), :]
        s = nt_dot(q2[...], keys)
        slot = kb - q_idx
        s = jnp.minimum(s.reshape(HEADS_PER_STEP, Q_TILE, K_TILE), cap[slot][None]).reshape(rows, K_TILE)
        s_scr[slot] = s
        m_acc[...] = jnp.maximum(m_acc[...], jnp.maximum(s[:, :128], s[:, 128:]))
        return 0

    lax.fori_loop(kb_low, kb_end, scores, 0)
    row_max = jnp.max(m_acc[...], axis=1, keepdims=True)
    m_acc[...] = jnp.broadcast_to(row_max, m_acc.shape)
    l_acc[...] = jnp.zeros_like(l_acc)
    d_acc[...] = jnp.zeros_like(d_acc)

    def exps(kb, _):
        vals = v_ref[pl.ds(pl.multiple_of((kb + base) * K_TILE, K_TILE), K_TILE), :]
        slot = kb - q_idx
        dp = nt_dot(do2[...], vals)
        m = m_acc[...]
        e0 = jnp.exp(s_scr[slot, :, :128] - m)
        e1 = jnp.exp(s_scr[slot, :, 128:] - m)
        s_scr[slot, :, :128] = e0
        s_scr[slot, :, 128:] = e1
        dp_scr[slot] = dp
        l_acc[...] += e0 + e1
        d_acc[...] += e0 * dp[:, :128] + e1 * dp[:, 128:]
        return 0

    lax.fori_loop(kb_low, kb_end, exps, 0)
    inv_l = 1.0 / jnp.sum(l_acc[...], axis=1, keepdims=True)
    delta = jnp.sum(d_acc[...], axis=1, keepdims=True) * inv_l
    l_acc[...] = jnp.broadcast_to(inv_l, l_acc.shape)
    d_acc[...] = jnp.broadcast_to(delta, d_acc.shape)
    o_acc[...] = jnp.zeros_like(o_acc)
    dq_acc[...] = jnp.zeros_like(dq_acc)

    def grads(kb, _):
        start = pl.multiple_of((kb + base) * K_TILE, K_TILE)
        keys = k_ref[pl.ds(start, K_TILE), :]
        vals = v_ref[pl.ds(start, K_TILE), :]
        slot = kb - q_idx
        inv = jnp.concatenate([l_acc[...], l_acc[...]], axis=1)
        dlt = jnp.concatenate([d_acc[...], d_acc[...]], axis=1)
        p = s_scr[slot] * inv
        ds = (p * (dp_scr[slot] - dlt)).astype(jnp.bfloat16)
        pb = p.astype(jnp.bfloat16)
        o_acc[...] += nn_dot(pb, vals)
        dq_acc[...] += nn_dot(ds, keys)
        dk_t[kb] += nn_dot(q2t[...], ds)
        dv_t[kb] += nn_dot(do2t[...], pb)
        return 0

    lax.fori_loop(kb_low, kb_end, grads, 0)

    for h in range(HEADS_PER_STEP):
        span = slice(h * Q_TILE, (h + 1) * Q_TILE)
        o_ref[:, h * HEAD_DIM:(h + 1) * HEAD_DIM] = o_acc[span, :].astype(jnp.bfloat16)
        dq = dq_acc[span, :].astype(jnp.bfloat16).astype(jnp.float32)
        low_half = dq[:, :128]
        turned = low_half * cos_ref[...] - pltpu.roll(low_half, 64, 1) * sin_ref[...]
        dq_ref[:, h * HEAD_DIM:h * HEAD_DIM + 128] = (turned * scale).astype(jnp.bfloat16)
        dq_ref[:, h * HEAD_DIM + 128:(h + 1) * HEAD_DIM] = (dq[:, 128:] * scale).astype(jnp.bfloat16)

    @pl.when(jnp.logical_and(q_idx == pl.num_programs(0) - 1, h_idx == pl.num_programs(1) - 1))
    def _():
        def flush(blk, _):
            rows_out = pl.ds(pl.multiple_of(blk * K_TILE, K_TILE), K_TILE)
            kb = blk - base
            inside = jnp.logical_and(kb >= 0, kb < dk_t.shape[0])

            @pl.when(inside)
            def _():
                dkv_ref[rows_out, :HEAD_DIM] = dk_t[kb].T
                dkv_ref[rows_out, HEAD_DIM:] = dv_t[kb].T

            @pl.when(jnp.logical_not(inside))
            def _():
                dkv_ref[rows_out, :] = jnp.zeros((K_TILE, 2 * HEAD_DIM), jnp.float32)

            return 0

        lax.fori_loop(0, dkv_ref.shape[0] // K_TILE, flush, 0)


def attention(q_lin, d_o, kv_all, low, base_blk, cos2, sin2):
    tokens, width = q_lin.shape
    span = kv_all.shape[0]
    n_q = tokens // Q_TILE
    step_cols = HEADS_PER_STEP * HEAD_DIM
    rows = HEADS_PER_STEP * Q_TILE
    slots = WINDOW // K_TILE + 1
    first_blk = low[::Q_TILE, 0] // K_TILE
    tile = pl.BlockSpec((Q_TILE, step_cols), lambda i, h, fb, bb: (i, h))
    k_spec = pl.BlockSpec((span, HEAD_DIM), lambda i, h, fb, bb: (0, 0))
    v_spec = pl.BlockSpec((span, HEAD_DIM), lambda i, h, fb, bb: (0, 1))
    local_blks = (WINDOW + tokens) // K_TILE
    side = pl.BlockSpec((Q_TILE, 128), lambda i, h, fb, bb: (i, 0))
    pairs = tokens * width // HEAD_DIM * WINDOW
    f32 = jnp.float32
    return pl.pallas_call(
        attention_kernel,
        out_shape=(jax.ShapeDtypeStruct((tokens, width), jnp.bfloat16),
                   jax.ShapeDtypeStruct((tokens, width), jnp.bfloat16),
                   jax.ShapeDtypeStruct((span, 2 * HEAD_DIM), f32)),
        grid_spec=pltpu.PrefetchScalarGridSpec(
            num_scalar_prefetch=2,
            grid=(n_q, width // step_cols),
            in_specs=[tile, tile, k_spec, v_spec, pl.BlockSpec((Q_TILE, 1), lambda i, h, fb, bb: (i, 0)), side, side],
            out_specs=[tile, tile, pl.BlockSpec((span, 2 * HEAD_DIM), lambda i, h, fb, bb: (0, 0))],
            scratch_shapes=[
                pltpu.VMEM((slots, Q_TILE, K_TILE), f32),
                pltpu.VMEM((slots, rows, K_TILE), f32),
                pltpu.VMEM((slots, rows, K_TILE), f32),
                pltpu.VMEM((rows, HEAD_DIM), jnp.bfloat16),
                pltpu.VMEM((rows, HEAD_DIM), jnp.bfloat16),
                pltpu.VMEM((HEAD_DIM, rows), jnp.bfloat16),
                pltpu.VMEM((HEAD_DIM, rows), jnp.bfloat16),
                pltpu.VMEM((rows, 128), f32),
                pltpu.VMEM((rows, 128), f32),
                pltpu.VMEM((rows, 128), f32),
                pltpu.VMEM((rows, HEAD_DIM), f32),
                pltpu.VMEM((rows, HEAD_DIM), f32),
                pltpu.VMEM((local_blks, HEAD_DIM, K_TILE), f32),
                pltpu.VMEM((local_blks, HEAD_DIM, K_TILE), f32),
            ]),
        compiler_params=pltpu.CompilerParams(
            dimension_semantics=("arbitrary", "arbitrary"), vmem_limit_bytes=60 * 1024 * 1024),
        cost_estimate=pl.CostEstimate(flops=12 * pairs * HEAD_DIM, bytes_accessed=32 * 1024 * 1024, transcendentals=pairs),
    )(first_blk, base_blk, q_lin, d_o, kv_all, kv_all, low, cos2, sin2)


def solution(mesh):
    row_spec = P("dp", "sp", None)
    tok_spec = P("dp", "sp")
    mat_spec = P(None, None)
    grad_mat = P("dp", None)
    n_sp = mesh.shape["sp"]
    f32, bf16 = jnp.float32, jnp.bfloat16

    def tn_dot(a, b):
        return lax.dot_general(a, b, (((0,), (0,)), ((), ())), preferred_element_type=f32).astype(bf16)

    def gather(a):
        return lax.all_gather(a, "sp", axis=0, tiled=True)

    def gather_chips(a):
        groups = [list(range(core, n_sp, 2)) for core in (0, 1)]
        return lax.all_gather(a, "sp", axis=0, tiled=True, axis_index_groups=groups)

    def swap(a, bit):
        return lax.ppermute(a, "sp", [(i, i ^ bit) for i in range(n_sp)])

    def tree_gather(a, me):
        rows = a.shape[0]
        half = rows // 2
        a_x, a_y, a_c = swap(a, 2), swap(a, 4), swap(a, 1)
        far = jnp.concatenate([swap(a_y[:half], 2), swap(a_x[half:], 4)], axis=0)
        mine = {0: a, 2: a_x, 4: a_y, 6: far}
        other = {0: a_c, 2: swap(a_x, 1), 4: swap(a_y, 1), 6: swap(far, 1)}
        out = jnp.zeros((n_sp * rows,) + a.shape[1:], a.dtype)
        for m, shard in mine.items():
            for bit, part in ((m, shard), (m ^ 1, other[m])):
                out = lax.dynamic_update_slice(out, part, ((me ^ bit) * rows,) + (0,) * (a.ndim - 1))
        return out

    def pair(core, own, got):
        out = jnp.zeros((2,) + own.shape, own.dtype)
        return put(put(out, own, core, 0), got, 1 - core, 0)

    def trade_halves(a, core):
        rows, half = a.shape[0], a.shape[1] // 2
        first, second = a[:, :half], a[:, half:]
        keep = jnp.where(core == 0, first, second)
        got = swap(jnp.where(core == 0, second, first), 1)
        return pair(core, keep, got).reshape(2 * rows, half)

    def tree_scatter_sum(a, me):
        rows = a.shape[0] // n_sp
        core, x_bit, y_bit = me & 1, (me >> 1) & 1, (me >> 2) & 1
        parts = a.reshape(n_sp // 2, 2, rows, a.shape[1])

        def pick(arr, idx, axis):
            return lax.dynamic_index_in_dim(arr, idx, axis, keepdims=False)

        got = swap(pick(parts, 1 - core, 1), 1)
        parts = pick(parts, core, 1) + got
        parts = parts.reshape(2, 2, rows, a.shape[1])
        half = rows // 2
        top, low = parts[:, :, :half], parts[:, :, half:]
        top = pick(top, x_bit, 1) + swap(pick(top, 1 - x_bit, 1), 2)
        low = pick(low, y_bit, 0) + swap(pick(low, 1 - y_bit, 0), 4)
        top = pick(top, y_bit, 0) + swap(pick(top, 1 - y_bit, 0), 4)
        low = pick(low, x_bit, 0) + swap(pick(low, 1 - x_bit, 0), 2)
        return jnp.concatenate([top, low], axis=0)

    def put(buf, part, core, col):
        return lax.dynamic_update_slice(buf, part[None], (core, 0, col))

    def step(x, seg_ids, positions, out_grad, norm_scale, w_q, w_k, w_v, w_o, b_o):
        tokens, width = x.shape[1], x.shape[2]
        heads_width = w_q.shape[1]
        me = lax.axis_index("sp")
        core = me & 1
        og = out_grad[0]
        og_all = gather(og)
        seg = seg_ids[0]
        seg_all = tree_gather(seg, me)

        x_f32 = x[0].astype(f32)
        normed, norm_pull = jax.vjp(rms_norm, x_f32, norm_scale.astype(f32))
        half = HEAD_DIM // 4
        inv_freq = ROPE_BASE ** (-(jnp.arange(half, dtype=f32) * 2.0 / (HEAD_DIM // 2)))
        angles = positions[0].astype(f32)[:, None] * inv_freq
        cos_a, sin_a = jnp.cos(angles), jnp.sin(angles)
        cos2 = jnp.concatenate([cos_a, cos_a], axis=1)
        sin2 = jnp.concatenate([-sin_a, sin_a], axis=1)

        keys = rotate(nn_dot(normed, w_k), cos2, sin2).astype(bf16)
        values = nn_dot(normed, w_v).astype(bf16)
        n_half = gather_chips(trade_halves(normed, core))
        kv_all = tree_gather(jnp.concatenate([keys, values], axis=1), me)

        base = me * tokens - WINDOW
        doc_start = jnp.sum((seg_all[None, :] < seg[:, None]).astype(jnp.int32), axis=1)
        low = jnp.maximum(doc_start - base, jnp.arange(tokens) + 1).astype(jnp.int32)[:, None]
        base_blk = (base // K_TILE).astype(jnp.int32).reshape(1)

        blanks = [jnp.ones(shape, bf16) for shape in ((2, heads_width // 2, width), (2, width // 2, heads_width))]
        *blanks, low = lax.optimization_barrier((*blanks, low))
        d_o = nt_dot(og, w_o).astype(bf16)
        q_lin = nn_dot(normed, w_q)
        o_tok, dq_lin, dkv_part = attention(q_lin, d_o, kv_all, low, base_blk, cos2, sin2)

        o_half = gather_chips(trade_halves(o_tok, core))
        cut = heads_width * 3 // 4
        dq_a = gather(dq_lin[:, :cut])
        dq_b = gather(dq_lin[:, cut:])

        block_out = (x_f32 + nn_dot(o_tok, w_o) + b_o.astype(f32)).astype(bf16)

        dkv = tree_scatter_sum(dkv_part, me).astype(bf16)
        dk_lin = rotate(dkv[:, :HEAD_DIM].astype(f32), cos2, -sin2).astype(bf16)
        dv_lin = dkv[:, HEAD_DIM:]
        dkv_all = tree_gather(jnp.concatenate([dk_lin, dv_lin], axis=1), me)

        d_normed = (nt_dot(dq_lin, w_q) + nt_dot(dk_lin, w_k) + nt_dot(dv_lin, w_v)).astype(bf16)
        dx_norm, gain_part = norm_pull(d_normed)
        x_grad = (og.astype(f32) + dx_norm).astype(bf16)
        small = jnp.stack([gain_part, jnp.sum(og, axis=0, dtype=f32)])
        for bit in (1, 2, 4):
            got = swap(small, bit)
            small = small + got
        small = small.astype(bf16)

        w_o_grad, w_q_grad = blanks

        def both(buf, part, col):
            buf = put(buf, part, core, col)
            return put(buf, swap(part, 1), 1 - core, col)

        o_rows = lax.optimization_barrier(tn_dot(o_half, og_all))
        w_o_grad = both(w_o_grad, o_rows, 0).reshape(heads_width, width)
        kv_rows = lax.optimization_barrier(tn_dot(n_half, dkv_all))
        w_kv_grad = pair(core, kv_rows, swap(kv_rows, 1)).reshape(width, 2 * HEAD_DIM)
        w_k_grad, w_v_grad = w_kv_grad[:, :HEAD_DIM], w_kv_grad[:, HEAD_DIM:]
        qa_rows = tn_dot(n_half, dq_a)
        qb_rows = tn_dot(n_half, dq_b)
        w_q_grad = put(put(w_q_grad, qa_rows, core, 0), qb_rows, core, cut)
        for rows, col in ((qa_rows, 0), (qb_rows, cut)):
            w_q_grad = put(w_q_grad, swap(rows, 1), 1 - core, col)
        w_q_grad = w_q_grad.reshape(width, heads_width)
        return (block_out[None], x_grad[None], small[0], w_q_grad, w_k_grad, w_v_grad, w_o_grad, small[1])

    return jax.shard_map(step, mesh=mesh,
                         in_specs=(row_spec, tok_spec, tok_spec, row_spec, P(None), mat_spec, mat_spec, mat_spec, mat_spec, P(None)),
                         out_specs=(row_spec, row_spec, P("dp"), grad_mat, grad_mat, grad_mat, grad_mat, P("dp")),
                         check_vma=False)
```
